32 devices in a mesh: band: 8 (over z, y), grid: 4 (over x, core).
Axes of the slice: x: 2, y: 2, z: 4, core: 2. Of those that a mesh axis runs over, the one named last changes fastest.
Arguments:
- orbitals: float32 [24, 64, 4096], P('band', 'grid'), may hold values from -6 to 6
- pair_mask: int32 [24, 24], replicated, may hold values from 0 to 1, as said below
Outputs:
- exchange_term: float32 [24, 64, 4096], P('band', 'grid')
The draws below stay inside these ranges and needn't reach their ends.
Inputs may be any that keep to these rules, and one draw needn't show every extreme that they name: pair_mask is symmetric; entries outside the candidate pairs of every block (and their transposes) are 0; each block has at most 12 candidate pairs with mask 1, and some block has exactly 12.
All inputs are finite; a program needn't handle non-finite values.
Results may differ from the reference program's by a relative error of at most 0.00027.
Values sent between devices are 32-bit elements; how exact they have to be, the bound alone decides.
A program may use at most 64 MiB of HBM per device.

```python
import math
import jax
import jax.numpy as jnp
import numpy as np
from jax import lax

NG = 64
ORB_DEV = 3
REACH = 2
NORB = 24
NCAND = 24
CAP = 12


def pair_table_drawn():
    entries = []
    for distance in range(REACH + 1):
        for leading_orbital in range(ORB_DEV):
            for second_orb in range(ORB_DEV):
                if distance > 0 or leading_orbital <= second_orb:
                    entries.append((leading_orbital, distance, second_orb))
    return np.array(entries, dtype=np.int32)


def draw_orbitals(key, part):
    full_shape = (NORB, NG, NG * NG)
    values_out = jax.random.normal(key, full_shape, jnp.float32)
    return jnp.clip(values_out, -6.0, 6.0)


def draw_pair_mask(key, part):
    pair_list = pair_table_drawn()
    groups = NORB // ORB_DEV
    key_counts, key_full, key_scores = jax.random.split(jax.random.fold_in(key, 17), 3)
    counts = jax.random.randint(key_counts, (groups,), 1, CAP + 1)
    full_group = jax.random.randint(key_full, (), 0, groups)
    counts = jnp.where(jnp.arange(groups, dtype=jnp.int32) == full_group, CAP, counts)
    scores = jax.random.randint(key_scores, (groups, NCAND), 0, 1 << 20) * NCAND + jnp.arange(NCAND, dtype=jnp.int32)[None, :]
    ranks = jnp.argsort(jnp.argsort(scores, axis=1), axis=1)
    live_flags = (ranks < counts[:, None]).astype(jnp.int32)
    group_ids = jnp.arange(groups, dtype=jnp.int32)[:, None]
    row_ids = group_ids * ORB_DEV + jnp.asarray(pair_list[:, 0])[None, :]
    col_ids = (group_ids + jnp.asarray(pair_list[:, 1])[None, :]) % groups * ORB_DEV + jnp.asarray(pair_list[:, 2])[None, :]
    mask_out = jnp.zeros((NORB, NORB), jnp.int32)
    mask_out = mask_out.at[row_ids.reshape(-1), col_ids.reshape(-1)].set(live_flags.reshape(-1))
    mask_out = mask_out.at[col_ids.reshape(-1), row_ids.reshape(-1)].set(live_flags.reshape(-1))
    return mask_out


def setup_inputs(seed: int = 0) -> dict:
    key_list = jax.random.split(jax.random.key(seed), 3)
    return {
        "orbitals": draw_orbitals(jax.random.fold_in(key_list[2], 71), 0),
        "pair_mask": draw_pair_mask(jax.random.fold_in(key_list[2], 71), 0),
    }


MIXING = 0.25
BOX_LENGTH = 16.0


def pair_table():
    entries = []
    for distance in range(REACH + 1):
        for leading_orbital in range(ORB_DEV):
            for second_orb in range(ORB_DEV):
                if distance > 0 or leading_orbital <= second_orb:
                    entries.append((leading_orbital, distance, second_orb))
    return np.array(entries, dtype=np.int32)


def poisson_green_kernel():
    positions = jnp.arange(NG, dtype=jnp.int32)
    signed_waves = jnp.where(positions < NG // 2, positions, positions - NG)
    squared = (signed_waves[:, None, None] ** 2 + signed_waves[None, :, None] ** 2
               + signed_waves[None, None, :] ** 2)
    safe_values = jnp.maximum(squared, 1).astype(jnp.float32)
    return jnp.where(squared > 0, jnp.float32(BOX_LENGTH * BOX_LENGTH / math.pi) / safe_values,
                     jnp.float32(0.0))


def reference(orbitals, pair_mask):
    groups = NORB // ORB_DEV
    pair_list = pair_table()
    band_ids = np.arange(groups, dtype=np.int32)[:, None]
    row_ids = (band_ids * ORB_DEV + pair_list[None, :, 0]).reshape(-1).astype(np.int32)
    col_ids = (((band_ids + pair_list[None, :, 1]) % groups) * ORB_DEV
               + pair_list[None, :, 2]).reshape(-1).astype(np.int32)
    weights = pair_mask[jnp.asarray(row_ids), jnp.asarray(col_ids)].astype(jnp.float32)
    cross_flags = jnp.asarray((row_ids != col_ids).astype(np.float32)).astype(jnp.float32)
    cubes = orbitals.reshape(NORB, NG, NG, NG)
    kernel = poisson_green_kernel()

    def one_pair(totals, pair_input):
        row_id, col_id, weight, cross_flag = pair_input
        first_cube = cubes[row_id]
        second_cube = cubes[col_id]
        potential = jnp.real(jnp.fft.ifftn(jnp.fft.fftn(first_cube * second_cube) * kernel))
        totals = totals.at[row_id].add(weight * potential * second_cube)
        totals = totals.at[col_id].add(weight * cross_flag * potential * first_cube)
        return totals, None

    totals, discarded_value = lax.scan(one_pair, jnp.zeros((NORB, NG, NG, NG), jnp.float32),
                              (jnp.asarray(row_ids).astype(jnp.int32), jnp.asarray(col_ids).astype(jnp.int32),
                               weights, cross_flags))
    return (-MIXING * totals).reshape(NORB, NG, NG * NG)
```

```python
import math

import jax
import jax.numpy as jnp
import numpy as np
from jax import lax
from jax.sharding import PartitionSpec as P

NG = 64
ORB_DEV = 3
REACH = 2
NCAND = 24
CAP = 12


MIXING = 0.25
BOX_LENGTH = 16.0
EXACT_PRECISION = lax.Precision.HIGH
CHUNKS = 3


def shifted(block, axis, distance):
    devices = range(lax.axis_size(axis))
    route = [((i - distance) % len(devices), i) for i in devices]
    return lax.ppermute(block, axis, route)


def pair_table():
    entries = []
    for distance in range(REACH + 1):
        for leading_orbital in range(ORB_DEV):
            for second_orb in range(ORB_DEV):
                if distance > 0 or leading_orbital <= second_orb:
                    entries.append((leading_orbital, distance, second_orb))
    return np.array(entries, dtype=np.int32)


def rotate_parts(values_in):
    half_width = values_in.shape[-1] // 2
    return jnp.concatenate([values_in[..., half_width:], -values_in[..., :half_width]], axis=-1)


def transform_axis(values_in, tables, formula, sweep_direction):
    cosine_table, sine_table = tables
    direct_part = jnp.einsum(formula, cosine_table, values_in, precision=EXACT_PRECISION)
    crossed_part = jnp.einsum(formula, sine_table, values_in, precision=EXACT_PRECISION)
    return direct_part + sweep_direction * rotate_parts(crossed_part)


def signed_frequency(positions):
    return jnp.where(positions < NG // 2, positions, positions - NG)


def coulomb_values(squared):
    safe_values = jnp.maximum(squared, 1).astype(jnp.float32)
    return jnp.where(squared > 0, BOX_LENGTH * BOX_LENGTH / math.pi / safe_values, 0.0)


def exchange(blocks):
    got = [blocks[0]]
    for step in range(1, len(blocks)):
        got.append(shifted(blocks[step], "grid", step))
    return got


def local(orbitals, pair_mask):
    orb_count, planes, cells = orbitals.shape
    groups = lax.axis_size("band")
    parts = lax.axis_size("grid")
    band_index = lax.axis_index("band")
    grid_index = lax.axis_index("grid")
    visits = [orbitals]
    for distance in range(1, REACH + 1):
        visits.append(shifted(orbitals, "band", -distance))
    flat_count = (REACH + 1) * orb_count
    doubled = []
    for visit in visits:
        cube = visit.reshape(orb_count, planes, NG, NG)
        doubled.append(jnp.concatenate([cube, cube], axis=-1))
    doubled = jnp.concatenate(doubled)

    pair_list = pair_table()
    first_all = jnp.asarray(pair_list[:, 0])
    offsets = jnp.asarray(pair_list[:, 1])
    second_all = jnp.asarray(pair_list[:, 2])
    row_ids = band_index * ORB_DEV + first_all
    col_ids = (band_index + offsets) % groups * ORB_DEV + second_all
    live = pair_mask[row_ids, col_ids]
    slot_of = jnp.cumsum(live) - 1
    fields = -(-CAP // (2 * CHUNKS)) * CHUNKS
    slots = jnp.arange(2 * fields, dtype=jnp.int32)
    taken = ((slot_of[None, :] == slots[:, None]) & (live[None, :] > 0)).astype(jnp.int32)
    first_ids = jnp.sum(taken * first_all[None, :], axis=1)
    slot_ids = jnp.sum(taken * (offsets * ORB_DEV + second_all)[None, :], axis=1)
    weights = jnp.sum(taken, axis=1).astype(jnp.float32)
    self_flags = (first_ids != slot_ids).astype(jnp.float32)

    def by_lane(ids, count, scale):
        hot = (ids[:, None] == jnp.arange(count, dtype=jnp.int32)[None, :]).astype(jnp.float32)
        hot = (hot * scale[:, None]).reshape(fields, 2, count, 1)
        halves = [jnp.broadcast_to(hot[:, h], (fields, count, NG)) for h in range(2)]
        return jnp.concatenate(halves, axis=-1)[:, :, None, None, :]

    owner_hot = by_lane(first_ids, orb_count, weights)
    visit_hot = by_lane(slot_ids, flat_count, weights * self_flags)
    ones = jnp.ones_like(weights)
    first_hot = by_lane(first_ids, orb_count, ones)
    slot_hot = by_lane(slot_ids, flat_count, ones)
    owner_hot, visit_hot, first_hot, slot_hot = lax.optimization_barrier(
        (owner_hot, visit_hot, first_hot, slot_hot))

    ids = np.arange(NG)
    angles = (ids[:, None] * ids[None, :] % NG) * (2.0 * np.pi / NG)
    cosine, sine = np.cos(angles), np.sin(angles)
    forward_complex = jnp.asarray(np.block([[cosine, -sine], [sine, cosine]]), jnp.float32)
    inverse_complex = jnp.asarray(np.block([[cosine, sine], [-sine, cosine]]), jnp.float32)
    inside = jnp.arange(planes, dtype=jnp.int32)

    def here(tables_of):
        every = np.stack([tables_of(place) for place in range(parts)]).astype(np.float32)
        return lax.dynamic_index_in_dim(jnp.asarray(every), grid_index, 0, keepdims=False)

    def order(place, sign, chunk, count):
        steps = (place + sign * np.arange(parts)) % parts
        depth = planes // count
        rows = steps[:, None] * planes + chunk * depth + np.arange(depth)[None, :]
        return rows.reshape(-1)

    def rows_table(sign, chunk=0, count=1):
        return tuple(here(lambda place: t[order(place, sign, chunk, count)]) for t in (cosine, sine))

    def cols_table(sign, chunk=0, count=1):
        return tuple(here(lambda place: t[:, order(place, sign, chunk, count)]) for t in (cosine, sine))

    send_tables = rows_table(1)
    recv_tables = cols_table(-1)
    waves_first = signed_frequency(jnp.arange(NG, dtype=jnp.int32))[:, None, None]
    waves_second = signed_frequency(grid_index * planes + inside)[None, :, None]
    waves_third = signed_frequency(jnp.arange(NG, dtype=jnp.int32))[None, None, :]
    kernel = coulomb_values(
        waves_first * waves_first + waves_second * waves_second + waves_third * waves_third
    ) / float(NG**3)
    kernel_pair = jnp.concatenate([kernel, kernel], axis=-1)
    left_half = jnp.arange(2 * NG, dtype=jnp.int32) < NG

    def pick(doubled, hot):
        picked = []
        for field in range(hot.shape[0]):
            total = hot[field, 0] * doubled[0]
            for orbital in range(1, hot.shape[1]):
                total = total + hot[field, orbital] * doubled[orbital]
            picked.append(total)
        return jnp.stack(picked)

    per_chunk = fields // CHUNKS
    chunk_first, chunk_second, sent = [], [], []
    for chunk in range(CHUNKS):
        span = slice(chunk * per_chunk, (chunk + 1) * per_chunk)
        leading, second = pick(doubled, first_hot[span]), pick(doubled, slot_hot[span])
        chunk_first.append(leading)
        chunk_second.append(second)
        spectrum = jnp.einsum("pxyz,zk->pxyk", leading * second, forward_complex,
                              precision=EXACT_PRECISION)
        spectrum = transform_axis(spectrum, send_tables, "ky,pxyc->pxkc", 1.0)
        sent.append(exchange([spectrum[:, :, s * planes:(s + 1) * planes] for s in range(parts)]))
    back = []
    for chunk in range(CHUNKS):
        columns = jnp.concatenate(sent[chunk], axis=1)
        columns = transform_axis(columns, recv_tables, "kx,pxyc->pkyc", 1.0)
        columns = columns * kernel_pair[None]
        columns = transform_axis(columns, send_tables, "kx,pxyc->pkyc", -1.0)
        back.append(exchange([columns[:, s * planes:(s + 1) * planes] for s in range(parts)]))
    owned_total = 0.0
    visit_total = 0.0
    for chunk in range(CHUNKS):
        returned = jnp.concatenate(back[chunk], axis=2)
        returned = transform_axis(returned, recv_tables, "ky,pxyc->pxkc", -1.0)
        potential = jnp.einsum("pxyc,ck->pxyk", returned, inverse_complex,
                               precision=EXACT_PRECISION)
        for field in range(per_chunk):
            index = chunk * per_chunk + field
            to_owner = potential[field] * chunk_second[chunk][field]
            to_visit = potential[field] * chunk_first[chunk][field]
            owner_row = owner_hot[index]
            visit_row = visit_hot[index]
            owned_total = owned_total + owner_row * to_owner[None]
            visit_total = visit_total + visit_row * to_visit[None]

    def folded(total):
        half = total[..., :NG] + total[..., NG:]
        return half.reshape(total.shape[0], planes, cells)

    owned = folded(owned_total + visit_total[:orb_count])
    for distance in range(REACH, 0, -1):
        away = folded(visit_total[distance * orb_count:(distance + 1) * orb_count])
        owned = owned + shifted(away, "band", distance)
    return -MIXING * owned


def solution(mesh):
    return jax.shard_map(
        local,
        mesh=mesh,
        in_specs=(P("band", "grid", None), P()),
        out_specs=P("band", "grid", None),
        check_vma=False,
    )
```
